256 devices in a mesh: sweep: 2 (over z), expert: 16 (over y, core), fsdp: 8 (over x).
Axes of the slice: x: 8, y: 8, z: 2, core: 2. Of those that a mesh axis runs over, the one named last changes fastest.
The devices are a block of a 8x8x16 slice.
Arguments:
- tokens: bfloat16 [32768, 2048], P(('sweep', 'expert', 'fsdp')), parts along dimension 0, may hold values from -6 to 6
- context: bfloat16 [32768, 2048], P(('sweep', 'expert', 'fsdp')), parts along dimension 0, may hold values from -6 to 6
- out_proj: bfloat16 [4096, 2048], P(('sweep', 'expert', 'fsdp')), parts along dimension 0, may hold values from -0.125 to 0.125
- norm_gain: float32 [4096], P('sweep'), parts along dimension 0, may hold values from 0.1 to 1.9
- router: bfloat16 [4096, 64], P('sweep'), parts along dimension 0, may hold values from -0.125 to 0.125
- expert_ids: int32 [32768, 2], P(('sweep', 'expert', 'fsdp')), parts along dimension 0, may hold values from 0 to 63, all different within a row; in each aligned block of 128 rows (0 to 127, 128 to 255, ...) at most 5 rows name the same one
- w_gate_up: bfloat16 [256, 2, 704, 2048], P(('sweep', 'expert', 'fsdp')), parts along dimension 0, may hold values from -0.125 to 0.125
- w_down: bfloat16 [256, 704, 2048], P(('sweep', 'expert', 'fsdp')), parts along dimension 0, may hold values from -0.15625 to 0.15625
Outputs:
- layer_out: bfloat16 [32768, 2048], P(('sweep', 'expert', 'fsdp')), parts along dimension 0
The draws below stay inside these ranges and needn't reach their ends.
There are 2 independent parts, one for each index of `sweep`. The reference program is written for one: setup_inputs(seed, part) draws one part's arguments, and reference() takes and returns one part's arrays. A program takes and returns all parts, laid end to end along the dimension named above; each array names one. Nothing has to cross between parts.
Inputs may be any that keep to these rules, and one draw needn't show every extreme that they name: `expert_ids`: each row names two different experts. Among the rows of one device no expert is named more than 5 times, a bound that some block reaches.
All inputs are finite; a program needn't handle non-finite values.
Results may differ from the reference program's by a relative error of at most 0.012.
Values may be sent and summed in bfloat16 or wider, within the bound.
No kernel may reach another device: no remote copies, remote signals or barrier semaphores. Data moves between devices by JAX's collectives and lax.ppermute only.
A program may use at most 64 MiB of HBM per device.

```python
import math
import jax
import jax.numpy as jnp
import numpy as np
from jax import lax

D = 2048
FF = 1408
EXPERTS = 64
TOK_DEV = 128
CAP = 5
TOKENS = 16384
N_EXPERT = 16
N_FSDP = 8


def block_scale(own_key, dims, cuts, least, high):
    def one(dim, blocks):
        steps = jax.random.uniform(jax.random.fold_in(jax.random.fold_in(own_key, 6), dim), (blocks,), jnp.float32, least / len(cuts), high / len(cuts))
        return jnp.repeat(jnp.exp(steps), dims[dim] // blocks).reshape((-1,) + (1,) * (len(dims) - dim - 1))

    factor_of = one(*cuts[0])
    for cut in cuts[1:]:
        factor_of = factor_of * one(*cut)
    return factor_of


def assign_block(own_key, own, number, rows, number_of, top, most, skew):
    order = jax.random.permutation(own_key, number_of)
    packed, ordinary = portions_of(number_of, rows * top, most, skew, True), portions_of(number_of, rows * top, most, skew, False)
    places = jnp.arange(number_of)

    def named(lengths, turn):
        used = int((lengths > 0).sum())
        fixed = max(1, used // 4)
        moved = fixed + (places - fixed + turn * (used - fixed)) % max(1, number_of - fixed)
        return jnp.zeros((number_of,), jnp.int32).at[order[jnp.where(places < fixed, places, moved)]].set(jnp.asarray(lengths, jnp.int32))

    lengths = jnp.where(number % 4 == 0, named(packed, number // 4), named(ordinary, number - number // 4 - 1))
    mixed = jax.random.permutation(jax.random.fold_in(own, 3), number_of)
    giver, receiver = mixed[0:number_of // 2 * 2:2], mixed[1:number_of // 2 * 2:2]
    margin = jnp.minimum(lengths[giver] - 1, most - lengths[receiver]) // 2
    margin = jnp.where((giver == order[0]) | (receiver == order[0]) | (lengths[receiver] == 0), 0, jnp.maximum(margin, 0))
    moved = jax.random.randint(jax.random.fold_in(own, 4), (number_of // 2,), 0, 1 << 20) % (margin + 1)
    lengths = lengths.at[giver].add(-moved).at[receiver].add(moved)
    items = jnp.searchsorted(jnp.cumsum(lengths), jnp.arange(rows * top), side="right").astype(jnp.int32)
    listing = items.reshape(top, rows).T
    listing = listing[jax.random.permutation(jax.random.fold_in(own, 1), rows)]
    turn = jax.random.randint(jax.random.fold_in(own, 2), (rows, 1), 0, top)
    return jnp.take_along_axis(listing, (jnp.arange(top)[None, :] + turn) % top, axis=1)


def portions_of(count, total, limit, skew, full):
    weights = [(1 << 20) // math.isqrt(standing ** skew) + 1 for standing in range(1, count + 1)]
    largest = limit if full else min(limit, max(-(-total // count), total * weights[0] // sum(weights)))
    least = 1 if total - largest >= count - 1 else 0
    counts, spare = [largest] + [least] * (count - 1), total - largest - least * (count - 1)
    while spare > 0:
        movable = [i for i in range(1, count) if counts[i] < largest] or [i for i in range(1, count) if counts[i] < limit]
        mass, left = sum([weights[i] for i in movable]), spare
        for i in movable:
            more = min(limit - counts[i], max(1, left * weights[i] // mass), spare)
            counts[i] = counts[i] + more
            spare = spare - more
    return np.array(counts)


def scatter_about(rng, shape, scale, most, split=(), held_as=jnp.bfloat16):
    entries = scale * jax.random.normal(rng, shape, jnp.float32)
    if split:
        entries = entries * block_scale(rng, shape, split, -0.22, 0.18)
    return jnp.clip(entries, -most, most).astype(held_as)


def setup_inputs(seed: int = 0, part: int = 0) -> dict:
    keys = jax.random.split(jax.random.key(seed), 9)
    part_keys = jax.random.split(jax.random.fold_in(keys[8], part), 9)
    tokens = scatter_about(part_keys[0], (TOKENS, D), 1.0, 6.0, ((0, 128),))
    context = scatter_about(part_keys[1], (TOKENS, D), 1.0, 6.0, ((0, 128),))
    out_proj = scatter_about(part_keys[2], (D, D), D ** -0.5, 0.125, ((0, 128),))
    norm_gain = jnp.clip(1.0 + 0.18 * jax.random.normal(part_keys[3], (D,), jnp.float32), 0.1, 1.9)
    router = scatter_about(part_keys[4], (D, EXPERTS), D ** -0.5, 0.125)
    expert_ids_keys = jax.random.split(jax.random.fold_in(part_keys[5], 1), TOKENS // TOK_DEV)
    expert_ids_turns = jax.random.permutation(jax.random.fold_in(part_keys[5], 3), TOKENS // TOK_DEV)
    expert_ids = jax.vmap(lambda own, number: assign_block(jax.random.fold_in(part_keys[5], 2), own, number, TOK_DEV, EXPERTS, 2, CAP, 2))(expert_ids_keys, expert_ids_turns).reshape((TOKENS, 2))
    w_gate_up = scatter_about(part_keys[6], (2 * EXPERTS, 2, FF // 2, D), D ** -0.5, 0.125, ((0, 128),))
    w_down = scatter_about(part_keys[7], (2 * EXPERTS, FF // 2, D), FF ** -0.5, 0.15625, ((0, 128),))
    return dict(tokens=tokens, context=context, out_proj=out_proj, norm_gain=norm_gain, router=router, expert_ids=expert_ids, w_gate_up=w_gate_up, w_down=w_down)


def reference(tokens, context, out_proj, norm_gain, router, expert_ids, w_gate_up, w_down):
    attended = jnp.dot(context, out_proj, preferred_element_type=jnp.float32)
    residual_in = (tokens.astype(jnp.float32) + attended).astype(jnp.bfloat16)
    widened = residual_in.astype(jnp.float32)
    inv_rms = lax.rsqrt(lax.optimization_barrier(jnp.mean(widened * widened, axis=1, keepdims=True)) + 1e-05)
    normed = (widened * inv_rms * norm_gain).astype(jnp.bfloat16)
    logits = jnp.dot(normed, router, preferred_element_type=jnp.float32)
    picked = jnp.take_along_axis(logits, expert_ids, axis=1)
    scores = jax.nn.sigmoid(picked)
    gate_vals = scores / lax.optimization_barrier(jnp.sum(scores, axis=1, keepdims=True))
    experts = EXPERTS
    blocks = N_EXPERT * N_FSDP
    ids_block = expert_ids.reshape(blocks, 2 * TOK_DEV)
    onehot = (ids_block[:, :, None] == jnp.arange(experts, dtype=jnp.int32)[None, None, :]).astype(jnp.int32)
    before = jnp.cumsum(onehot, axis=1) - onehot
    places = lax.optimization_barrier(jnp.sum(before * onehot, axis=2))
    block_of = jnp.arange(blocks, dtype=jnp.int32)[:, None]
    slot_index = ((ids_block * blocks + block_of) * CAP + places).reshape(-1).astype(jnp.int32)
    assign = jnp.arange(2 * TOKENS, dtype=jnp.int32)
    table_tok = jnp.full((experts * blocks * CAP,), TOKENS, jnp.int32).at[slot_index].set(assign // 2)
    table_gate = jnp.zeros((experts * blocks * CAP,), jnp.float32).at[slot_index].set(gate_vals.reshape(-1))
    padded = jnp.concatenate([normed, jnp.zeros((1, D), jnp.bfloat16)], axis=0)
    half_units = FF // 2

    def one_expert(running, inputs):
        slot_tokens, slot_gates, gate_up_w, down_w = inputs
        taken = padded[slot_tokens]
        total = jnp.zeros((taken.shape[0], D), jnp.float32)
        for half in range(2):
            gate_val = jnp.dot(taken, gate_up_w[half, 0].T, preferred_element_type=jnp.float32)
            up_val = jnp.dot(taken, gate_up_w[half, 1].T, preferred_element_type=jnp.float32)
            hidden = (jax.nn.silu(gate_val) * up_val).astype(jnp.bfloat16)
            piece = jnp.dot(hidden, down_w[half], preferred_element_type=jnp.float32).astype(jnp.bfloat16)
            piece = lax.optimization_barrier(piece)
            total = total + piece.astype(jnp.float32)
        combined = lax.optimization_barrier(total.astype(jnp.bfloat16)).astype(jnp.float32)
        running = running.at[slot_tokens].add(slot_gates[:, None] * combined)
        return (running, None)
    start_acc = jnp.zeros((TOKENS + 1, D), jnp.float32)
    running, unused = lax.scan(one_expert, start_acc, (table_tok.reshape(experts, -1), table_gate.reshape(experts, -1), w_gate_up.reshape(experts, 2, 2, half_units, D), w_down.reshape(experts, 2, half_units, D)))
    return (widened + running[:TOKENS]).astype(jnp.bfloat16)
```

```python
import functools

import jax
import jax.numpy as jnp
from jax import lax
from jax.experimental import pallas as pl
from jax.experimental.pallas import tpu as pltpu
from jax.sharding import PartitionSpec as P

eps_norm = 1e-05
LANES = 128

VMEM = pltpu.VMEM
SMEM = pltpu.SMEM


def whole(space):
    return pl.BlockSpec(memory_space=space)


def slot_places(expert_ids, experts):
    flat_ids = expert_ids.reshape(-1)
    onehot = (flat_ids[:, None] == jnp.arange(experts, dtype=jnp.int32)[None, :]).astype(jnp.int32)
    before = jnp.cumsum(onehot, axis=0) - onehot
    places = jnp.sum(before * onehot, axis=1)
    return (flat_ids, places)


def front_kernel(index_a, index_b, context, proj, tokens, gain, router, ids, box_a, box_b, kept, gates, res, tiles):
    step = pl.program_id(0)
    rows, wide = res.shape
    part = proj.shape[1]
    chunks = wide // LANES
    attended = jnp.dot(context[...], proj[...], preferred_element_type=jnp.float32)
    summed = (tokens[...].astype(jnp.float32) + attended).astype(jnp.bfloat16)
    res[:, pl.ds(pl.multiple_of(step * part, part), part)] = summed.astype(jnp.float32)

    @pl.when(step == pl.num_programs(0) - 1)
    def _():
        value = res[...]
        inv_rms = lax.rsqrt(jnp.mean(value * value, axis=1, keepdims=True) + eps_norm)
        for c in range(chunks):
            tiles[pl.ds(c, rows, stride=chunks), :] = value[:, c * LANES : (c + 1) * LANES]
        kept[...] = tiles[...].reshape(rows, chunks, LANES).astype(jnp.bfloat16)
        normed = (value * inv_rms * gain[...]).astype(jnp.bfloat16)
        logits = jnp.dot(normed, router[...], preferred_element_type=jnp.float32)
        lanes = lax.broadcasted_iota(jnp.int32, logits.shape, 1)
        scores = []
        for k in range(2):
            hit = lanes == ids[:, k : k + 1]
            picked = jnp.sum(jnp.where(hit, logits, 0.0), axis=1, keepdims=True)
            scores.append(jax.nn.sigmoid(picked))
        total = scores[0] + scores[1]
        gates[:, 0:1] = scores[0] / total
        gates[:, 1:2] = scores[1] / total
        wider = normed.astype(jnp.float32)
        for c in range(chunks):
            tiles[pl.ds(c, rows, stride=chunks), :] = wider[:, c * LANES : (c + 1) * LANES]
        box_a[...] = jnp.zeros_like(box_a)
        box_b[...] = jnp.zeros_like(box_b)
        half = chunks // 2

        def place(t, carry):
            start = pl.multiple_of(t * chunks, chunks)
            first = tiles[pl.ds(start, half), :].astype(jnp.bfloat16)
            second = tiles[pl.ds(start + half, half), :].astype(jnp.bfloat16)
            for k in range(2):
                box_a[index_a[2 * t + k]] = first
                box_b[index_b[2 * t + k]] = second
            return carry

        lax.fori_loop(0, rows, place, 0, unroll=4)


def front(index_a, index_b, context, proj, tokens, gain, router, ids, slots):
    rows, wide = tokens.shape
    part = wide // 4
    half = wide // LANES // 2
    box = jax.ShapeDtypeStruct((slots, half, LANES), jnp.bfloat16)
    fixed = lambda shape: pl.BlockSpec(shape, lambda n: (0,) * len(shape))
    return pl.pallas_call(
        front_kernel,
        grid=(wide // part,),
        in_specs=[
            whole(SMEM),
            whole(SMEM),
            fixed(context.shape),
            pl.BlockSpec((proj.shape[0], part), lambda n: (0, n)),
            pl.BlockSpec((rows, part), lambda n: (0, n)),
            fixed(gain.shape),
            fixed(router.shape),
            fixed(ids.shape),
        ],
        out_specs=[fixed(box.shape), fixed(box.shape), fixed((rows, 2 * half, LANES)), fixed((rows, 2))],
        out_shape=[
            box,
            box,
            jax.ShapeDtypeStruct((rows, 2 * half, LANES), jnp.bfloat16),
            jax.ShapeDtypeStruct((rows, 2), jnp.float32),
        ],
        scratch_shapes=[VMEM((rows, wide), jnp.float32), VMEM((rows * 2 * half, LANES), jnp.float32)],
        cost_estimate=pl.CostEstimate(
            flops=2 * rows * wide * wide, bytes_accessed=2 * wide * wide, transcendentals=0
        ),
    )(index_a, index_b, context, proj, tokens, gain, router, ids)


def fill_rows(blocks, lhs, tiles):
    for b, block in enumerate(blocks):
        rows, chunks, _ = block.shape
        tiles[...] = block[...].astype(jnp.float32).reshape(rows * chunks, LANES)
        for c in range(chunks):
            lhs[b * rows : (b + 1) * rows, c * LANES : (c + 1) * LANES] = tiles[
                pl.ds(c, rows, stride=chunks), :
            ].astype(jnp.bfloat16)


def spill_rows(value, blocks, tiles, start):
    rows, chunks, _ = blocks[0].shape
    for b in range(value.shape[0] // rows):
        for c in range(chunks):
            tiles[pl.ds(c, rows, stride=chunks), :] = value[b * rows : (b + 1) * rows, c * LANES : (c + 1) * LANES]
        blocks[start + b][...] = tiles[...].reshape(rows, chunks, LANES).astype(jnp.bfloat16)


def dot_t(lhs, rhs):
    return lax.dot_general(lhs, rhs, (((1,), (1,)), ((), ())), preferred_element_type=jnp.float32)


def gate_first_kernel(*refs):
    blocks, (weight, out, lhs, tiles) = refs[:8], refs[8:]
    fill_rows(blocks, lhs, tiles)
    for k in range(2):
        out[k] = dot_t(lhs[...], weight[0, k])


def gate_second_kernel(*refs):
    blocks, (weight, down, gate_up, hidden), outs, (lhs, tiles) = refs[:8], refs[8:12], refs[12:20], refs[20:]
    fill_rows(blocks, lhs, tiles)
    gate = gate_up[0] + dot_t(lhs[...], weight[0, 0])
    up = gate_up[1] + dot_t(lhs[...], weight[0, 1])
    hidden[...] = (gate / (1.0 + jnp.exp(-gate)) * up).astype(jnp.bfloat16)
    value = jnp.dot(hidden[...], down[0], preferred_element_type=jnp.float32)
    value = value.astype(jnp.bfloat16).astype(jnp.float32)
    spill_rows(value, outs, tiles, 0)


def down_second_kernel(*refs):
    (hidden, down), outs, (tiles,) = refs[:2], refs[2:10], refs[10:]
    value = jnp.dot(hidden[...], down[0], preferred_element_type=jnp.float32)
    value = value.astype(jnp.bfloat16).astype(jnp.float32)
    spill_rows(value, outs, tiles, 0)


def experts_first(blocks, w_gate_up):
    rows, chunks, _ = blocks[0].shape
    total, depth, units = rows * len(blocks), chunks * LANES, w_gate_up.shape[2]
    return pl.pallas_call(
        gate_first_kernel,
        grid=(1,),
        in_specs=[whole(VMEM)] * 8 + [pl.BlockSpec((1, 2, units, depth), lambda n: (0, 0, 0, 0))],
        out_specs=pl.BlockSpec((2, total, units), lambda n: (0, 0, 0)),
        out_shape=jax.ShapeDtypeStruct((2, total, units), jnp.float32),
        scratch_shapes=[VMEM((total, depth), jnp.bfloat16), VMEM((rows * chunks, LANES), jnp.float32)],
        cost_estimate=pl.CostEstimate(
            flops=4 * total * depth * units, bytes_accessed=4 * units * depth, transcendentals=0
        ),
    )(*blocks, w_gate_up)


def experts_second(blocks, w_gate_up, w_down, gate_up):
    rows, chunks, _ = blocks[0].shape
    total, depth, units = rows * len(blocks), chunks * LANES, w_gate_up.shape[2]
    got = pl.pallas_call(
        gate_second_kernel,
        grid=(1,),
        in_specs=[whole(VMEM)] * 8
        + [
            pl.BlockSpec((1, 2, units, depth), lambda n: (0, 0, 0, 1)),
            pl.BlockSpec((1, units, depth), lambda n: (0, 0, 0)),
            pl.BlockSpec((2, total, units), lambda n: (0, 0, 0)),
        ],
        out_specs=[pl.BlockSpec((total, units), lambda n: (0, 0))] + [whole(VMEM)] * 8,
        out_shape=[jax.ShapeDtypeStruct((total, units), jnp.bfloat16)]
        + [jax.ShapeDtypeStruct(b.shape, b.dtype) for b in blocks],
        scratch_shapes=[VMEM((total, depth), jnp.bfloat16), VMEM((rows * chunks, LANES), jnp.float32)],
        cost_estimate=pl.CostEstimate(
            flops=6 * total * depth * units, bytes_accessed=6 * units * depth, transcendentals=total * units
        ),
    )(*blocks, w_gate_up, w_down, gate_up)
    return got[0], got[1:]


def experts_third(hidden, w_down, like):
    rows, chunks, _ = like[0].shape
    total, units = hidden.shape
    depth = chunks * LANES
    return pl.pallas_call(
        down_second_kernel,
        grid=(1,),
        in_specs=[whole(VMEM), pl.BlockSpec((1, units, depth), lambda n: (0, 0, 1))],
        out_specs=[whole(VMEM)] * 8,
        out_shape=[jax.ShapeDtypeStruct(b.shape, b.dtype) for b in like],
        scratch_shapes=[VMEM((rows * chunks, LANES), jnp.float32)],
        cost_estimate=pl.CostEstimate(
            flops=2 * total * depth * units, bytes_accessed=2 * units * depth, transcendentals=0
        ),
    )(hidden, w_down)


def back_kernel(index_a, index_b, gates, from_a, from_b, kept, out, tiles):
    rows, chunks, _ = kept.shape
    half = chunks // 2

    def token(t, carry):
        start = pl.multiple_of(t * chunks, chunks)
        value = kept[t].astype(jnp.float32)
        first, second = value[:half], value[half:]
        for k in range(2):
            gate = gates[2 * t + k]
            first = first + gate * from_a[index_a[2 * t + k]].astype(jnp.float32)
            second = second + gate * from_b[index_b[2 * t + k]].astype(jnp.float32)
        tiles[pl.ds(start, half), :] = first
        tiles[pl.ds(start + half, half), :] = second
        return carry

    lax.fori_loop(0, rows, token, 0, unroll=4)
    for c in range(chunks):
        out[:, c * LANES : (c + 1) * LANES] = tiles[pl.ds(c, rows, stride=chunks), :].astype(jnp.bfloat16)


def back(index_a, index_b, gates, from_a, from_b, kept):
    rows, chunks, _ = kept.shape
    return pl.pallas_call(
        back_kernel,
        in_specs=[whole(SMEM)] * 3 + [whole(VMEM)] * 3,
        out_specs=whole(VMEM),
        out_shape=jax.ShapeDtypeStruct((rows, chunks * LANES), jnp.bfloat16),
        scratch_shapes=[VMEM((rows * chunks, LANES), jnp.float32)],
        cost_estimate=pl.CostEstimate(flops=1 << 20, bytes_accessed=1 << 22, transcendentals=0),
    )(index_a, index_b, gates, from_a, from_b, kept)


def on_device(tokens, context, out_proj, norm_gain, router, expert_ids, w_gate_up, w_down):
    rows_here, width = tokens.shape
    columns = lax.axis_size("expert")
    members = lax.axis_size("fsdp")
    experts = columns * members // 2
    group = members // 2
    slot_cap = 5 * rows_here // (2 * experts)
    slots = experts * slot_cap
    half = width // LANES // 2
    assert group == 4

    def shift(even, odd):
        return [(i, (i + (odd if i % 2 else even)) % members) for i in range(members)]

    out_hops = (shift(-1, 1), shift(2, -2), shift(-3, 3))
    back_hops = tuple([(b, a) for a, b in hop] for hop in out_hops)
    swap = [(i, i ^ 1) for i in range(members)]

    def spread(blocks, hops):
        return [blocks[0]] + [lax.ppermute(b, "fsdp", hop) for b, hop in zip(blocks[1:], hops)]

    def exchange(blocks):
        return [lax.ppermute(b, "fsdp", swap) for b in blocks]

    def across(boxes):
        return lax.all_to_all(boxes, "expert", split_axis=0, concat_axis=0, tiled=True)

    block_shape = (columns * slot_cap, half, LANES)

    def split(boxes):
        parts = boxes.reshape(columns, group, slot_cap, half, LANES)
        return [parts[:, m].reshape(block_shape) for m in range(group)]

    def join(blocks):
        parts = [b.reshape(columns, 1, slot_cap, half, LANES) for b in blocks]
        return jnp.concatenate(parts, axis=1).reshape(columns, group * slot_cap, half, LANES)

    def add_halves(own, other):
        return [(a.astype(jnp.float32) + b.astype(jnp.float32)).astype(jnp.bfloat16) for a, b in zip(own, other)]

    flat_ids, places = slot_places(expert_ids, experts)
    here = lax.axis_index("fsdp")
    odd = here % 2
    away = (flat_ids % group - here // 2) % group
    message = jnp.where(away == 0, 0, jnp.where(away == 2, 3, jnp.where((away == 1) == (odd == 0), 2, 1)))
    column = flat_ids // group
    index_a = ((column * group + message) * slot_cap + places).astype(jnp.int32)
    index_b = ((message * columns + column) * slot_cap + places).astype(jnp.int32)

    proj = lax.all_gather(out_proj, ("expert", "fsdp"), axis=0, tiled=True)
    box_a, box_b, kept, gates = front(
        index_a, index_b, context, proj, tokens, norm_gain.reshape(1, width), router, expert_ids, slots
    )

    near_b = spread(list(box_b.reshape((group,) + block_shape)), out_hops)
    over_a = across(box_a.reshape(columns, group * slot_cap, half, LANES))
    near_a = spread(split(over_a), out_hops)
    far_a = exchange(near_a)
    near_b = split(across(join(near_b)))
    far_b = exchange(near_b)

    gate_up = experts_first(near_a + far_a, w_gate_up)
    hidden, made_a = experts_second(near_b + far_b, w_gate_up, w_down, gate_up)
    made_b = experts_third(hidden, w_down, made_a)

    sum_a = add_halves(made_a[:4], exchange(made_a[4:]))
    sum_b = add_halves(made_b[:4], exchange(made_b[4:]))
    done_a = across(join(spread(sum_a, back_hops))).reshape(slots, half, LANES)
    done_b = jnp.concatenate(spread(split(across(join(sum_b))), back_hops), axis=0)
    return back(index_a, index_b, gates.reshape(-1), done_a, done_b, kept)


def solution(mesh):
    rows = P(("sweep", "expert", "fsdp"), None)
    return jax.shard_map(
        on_device,
        mesh=mesh,
        in_specs=(
            rows,
            rows,
            rows,
            P("sweep"),
            P("sweep", None),
            rows,
            P(("sweep", "expert", "fsdp"), None, None, None),
            P(("sweep", "expert", "fsdp"), None, None),
        ),
        out_specs=rows,
        check_vma=False,
    )
```

```python
import functools

import jax
import jax.numpy as jnp
from jax import lax
from jax.experimental import pallas as pl
from jax.experimental.pallas import tpu as pltpu
from jax.sharding import PartitionSpec as P


eps_norm = 1e-05
LANES = 128

VMEM = pltpu.VMEM
SMEM = pltpu.SMEM


def whole(space):
    return pl.BlockSpec(memory_space=space)


def slot_places(expert_ids, experts):
    flat_ids = expert_ids.reshape(-1)
    onehot = (flat_ids[:, None] == jnp.arange(experts, dtype=jnp.int32)[None, :]).astype(jnp.int32)
    before = jnp.cumsum(onehot, axis=0) - onehot
    places = jnp.sum(before * onehot, axis=1)
    return (flat_ids, places)


def front_kernel(index_a, index_b, odd, mine, other, gain, router, ids, box_a, box_b, kept, gates, tiles):
    rows, depth = mine.shape
    chunks = 2 * depth // LANES
    half = chunks // 2
    swapped = odd[0] == 1
    own, got = mine[...].astype(jnp.float32), other[...].astype(jnp.float32)
    parts = (jnp.where(swapped, got, own), jnp.where(swapped, own, got))
    squares = sum(jnp.sum(p * p, axis=1, keepdims=True) for p in parts)
    inv_rms = lax.rsqrt(squares / (2 * depth) + eps_norm)
    for c in range(chunks):
        lane = c % half * LANES
        tiles[pl.ds(c, rows, stride=chunks), :] = parts[c // half][:, lane : lane + LANES]
    kept[...] = tiles[...].reshape(rows, chunks, LANES).astype(jnp.bfloat16)
    normed = [
        (p * inv_rms * gain[:, h * depth : (h + 1) * depth]).astype(jnp.bfloat16) for h, p in enumerate(parts)
    ]
    logits = sum(
        jnp.dot(p, router[h * depth : (h + 1) * depth, :], preferred_element_type=jnp.float32)
        for h, p in enumerate(normed)
    )
    lanes = lax.broadcasted_iota(jnp.int32, logits.shape, 1)
    scores = []
    for k in range(2):
        hit = lanes == ids[:, k : k + 1]
        picked = jnp.sum(jnp.where(hit, logits, 0.0), axis=1, keepdims=True)
        scores.append(jax.nn.sigmoid(picked))
    total = scores[0] + scores[1]
    gates[:, 0:1] = scores[0] / total
    gates[:, 1:2] = scores[1] / total
    wider = [p.astype(jnp.float32) for p in normed]
    for c in range(chunks):
        lane = c % half * LANES
        tiles[pl.ds(c, rows, stride=chunks), :] = wider[c // half][:, lane : lane + LANES]
    box_a[...] = jnp.zeros_like(box_a)
    box_b[...] = jnp.zeros_like(box_b)

    def place(t, carry):
        start = pl.multiple_of(t * chunks, chunks)
        first = tiles[pl.ds(start, half), :].astype(jnp.bfloat16)
        second = tiles[pl.ds(start + half, half), :].astype(jnp.bfloat16)
        for k in range(2):
            box_a[index_a[2 * t + k]] = first
            box_b[index_b[2 * t + k]] = second
        return carry

    lax.fori_loop(0, rows, place, 0, unroll=4)


def front(index_a, index_b, odd, mine, other, gain, router, ids, slots):
    rows, depth = mine.shape
    half = depth // LANES
    box = jax.ShapeDtypeStruct((slots, half, LANES), jnp.bfloat16)
    return pl.pallas_call(
        front_kernel,
        in_specs=[whole(SMEM)] * 3 + [whole(VMEM)] * 5,
        out_specs=[whole(VMEM)] * 4,
        out_shape=[
            box,
            box,
            jax.ShapeDtypeStruct((rows, 2 * half, LANES), jnp.bfloat16),
            jax.ShapeDtypeStruct((rows, 2), jnp.float32),
        ],
        scratch_shapes=[VMEM((rows * 2 * half, LANES), jnp.float32)],
        cost_estimate=pl.CostEstimate(flops=1 << 24, bytes_accessed=1 << 23, transcendentals=0),
    )(index_a, index_b, odd, mine, other, gain, router, ids)


def fill_blocks(blocks, lhs, tiles):
    for b, block in enumerate(blocks):
        rows, chunks, _ = block.shape
        tiles[pl.ds(b * rows * chunks, rows * chunks), :] = block[...].astype(jnp.float32).reshape(rows * chunks, LANES)
    unpack(lhs, tiles, chunks)


def fill_boxes(boxes, lhs, tiles, columns, group):
    rows, chunks, _ = boxes[0].shape
    cap = rows // (columns * group)
    for b, box in enumerate(boxes):
        for col in range(columns):
            for m in range(group):
                source = (col * group + m) * cap
                target = b * rows + (m * columns + col) * cap
                piece = box[source : source + cap].astype(jnp.float32)
                tiles[target * chunks : (target + cap) * chunks, :] = piece.reshape(cap * chunks, LANES)
    unpack(lhs, tiles, chunks)


def unpack(lhs, tiles, chunks):
    rows = lhs.shape[0]
    for c in range(chunks):
        lhs[:, c * LANES : (c + 1) * LANES] = tiles[pl.ds(c, rows, stride=chunks), :].astype(jnp.bfloat16)


def pack(value, tiles, chunks):
    rows = value.shape[0]
    rounded = value.astype(jnp.bfloat16).astype(jnp.float32)
    for c in range(chunks):
        tiles[pl.ds(c, rows, stride=chunks), :] = rounded[:, c * LANES : (c + 1) * LANES]


def empty_blocks(blocks, tiles):
    for b, block in enumerate(blocks):
        rows, chunks, _ = block.shape
        piece = tiles[b * rows * chunks : (b + 1) * rows * chunks, :]
        block[...] = piece.reshape(rows, chunks, LANES).astype(jnp.bfloat16)


def empty_boxes(boxes, tiles, columns, group):
    rows, chunks, _ = boxes[0].shape
    cap = rows // (columns * group)
    for b, box in enumerate(boxes):
        for col in range(columns):
            for m in range(group):
                target = (col * group + m) * cap
                source = b * rows + (m * columns + col) * cap
                piece = tiles[source * chunks : (source + cap) * chunks, :]
                box[target : target + cap] = piece.reshape(cap, chunks, LANES).astype(jnp.bfloat16)


def dot_t(lhs, rhs):
    return lax.dot_general(lhs, rhs, (((1,), (1,)), ((), ())), preferred_element_type=jnp.float32)


def gate_first_kernel(*refs):
    blocks, (weight, out, lhs, tiles) = refs[:8], refs[8:]
    fill_blocks(blocks, lhs, tiles)
    for k in range(2):
        out[k] = dot_t(lhs[...], weight[0, k])


def gate_second_kernel(columns, group, *refs):
    boxes, (weight, down, gate_up, hidden), outs, (lhs, tiles) = refs[:2], refs[2:6], refs[6:8], refs[8:]
    fill_boxes(boxes, lhs, tiles, columns, group)
    gate = gate_up[0] + dot_t(lhs[...], weight[0, 0])
    up = gate_up[1] + dot_t(lhs[...], weight[0, 1])
    hidden[...] = (gate / (1.0 + jnp.exp(-gate)) * up).astype(jnp.bfloat16)
    pack(jnp.dot(hidden[...], down[0], preferred_element_type=jnp.float32), tiles, outs[0].shape[1])
    empty_boxes(outs, tiles, columns, group)


def down_second_kernel(hidden, down, *refs):
    outs, (tiles,) = refs[:-1], refs[-1:]
    pack(jnp.dot(hidden[...], down[0], preferred_element_type=jnp.float32), tiles, outs[0].shape[1])
    empty_blocks(outs, tiles)


def experts_first(blocks, w_gate_up):
    rows, chunks, _ = blocks[0].shape
    total, depth, units = rows * len(blocks), chunks * LANES, w_gate_up.shape[2]
    return pl.pallas_call(
        gate_first_kernel,
        grid=(1,),
        in_specs=[whole(VMEM)] * 8 + [pl.BlockSpec((1, 2, units, depth), lambda n: (0, 0, 0, 0))],
        out_specs=pl.BlockSpec((2, total, units), lambda n: (0, 0, 0)),
        out_shape=jax.ShapeDtypeStruct((2, total, units), jnp.float32),
        scratch_shapes=[VMEM((total, depth), jnp.bfloat16), VMEM((total * chunks, LANES), jnp.float32)],
        cost_estimate=pl.CostEstimate(
            flops=4 * total * depth * units, bytes_accessed=4 * units * depth, transcendentals=0
        ),
    )(*blocks, w_gate_up)


def experts_second(boxes, w_gate_up, w_down, gate_up, columns, group):
    rows, chunks, _ = boxes[0].shape
    total, depth, units = rows * len(boxes), chunks * LANES, w_gate_up.shape[2]
    box = jax.ShapeDtypeStruct(boxes[0].shape, jnp.bfloat16)
    return pl.pallas_call(
        functools.partial(gate_second_kernel, columns, group),
        grid=(1,),
        in_specs=[whole(VMEM)] * 2
        + [
            pl.BlockSpec((1, 2, units, depth), lambda n: (0, 0, 0, 1)),
            pl.BlockSpec((1, units, depth), lambda n: (0, 0, 0)),
            whole(VMEM),
        ],
        out_specs=[whole(VMEM)] * 3,
        out_shape=[jax.ShapeDtypeStruct((total, units), jnp.bfloat16), box, box],
        scratch_shapes=[VMEM((total, depth), jnp.bfloat16), VMEM((total * chunks, LANES), jnp.float32)],
        cost_estimate=pl.CostEstimate(
            flops=6 * total * depth * units, bytes_accessed=6 * units * depth, transcendentals=total * units
        ),
    )(*boxes, w_gate_up, w_down, gate_up)


def experts_third(hidden, w_down, like):
    total, units = hidden.shape
    chunks = like[0].shape[1]
    depth = chunks * LANES
    return pl.pallas_call(
        down_second_kernel,
        grid=(1,),
        in_specs=[whole(VMEM), pl.BlockSpec((1, units, depth), lambda n: (0, 0, 1))],
        out_specs=[whole(VMEM)] * len(like),
        out_shape=[jax.ShapeDtypeStruct(b.shape, b.dtype) for b in like],
        scratch_shapes=[VMEM((total * chunks, LANES), jnp.float32)],
        cost_estimate=pl.CostEstimate(
            flops=2 * total * depth * units, bytes_accessed=2 * units * depth, transcendentals=0
        ),
    )(hidden, w_down)


def back_kernel(index_a, index_b, gates, from_a, from_b, kept, out, tiles):
    rows, chunks, _ = kept.shape
    half = chunks // 2

    def token(t, carry):
        start = pl.multiple_of(t * chunks, chunks)
        value = kept[t].astype(jnp.float32)
        first, second = value[:half], value[half:]
        for k in range(2):
            gate = gates[2 * t + k]
            first = first + gate * from_a[index_a[2 * t + k]].astype(jnp.float32)
            second = second + gate * from_b[index_b[2 * t + k]].astype(jnp.float32)
        tiles[pl.ds(start, half), :] = first
        tiles[pl.ds(start + half, half), :] = second
        return carry

    lax.fori_loop(0, rows, token, 0, unroll=4)
    for c in range(chunks):
        out[:, c * LANES : (c + 1) * LANES] = tiles[pl.ds(c, rows, stride=chunks), :].astype(jnp.bfloat16)


def back(index_a, index_b, gates, from_a, from_b, kept):
    rows, chunks, _ = kept.shape
    return pl.pallas_call(
        back_kernel,
        in_specs=[whole(SMEM)] * 3 + [whole(VMEM)] * 3,
        out_specs=whole(VMEM),
        out_shape=jax.ShapeDtypeStruct((rows, chunks * LANES), jnp.bfloat16),
        scratch_shapes=[VMEM((rows * chunks, LANES), jnp.float32)],
        cost_estimate=pl.CostEstimate(flops=1 << 20, bytes_accessed=1 << 22, transcendentals=0),
    )(index_a, index_b, gates, from_a, from_b, kept)


def on_device(tokens, context, out_proj, norm_gain, router, expert_ids, w_gate_up, w_down):
    rows_here, width = tokens.shape
    columns = lax.axis_size("expert")
    members = lax.axis_size("fsdp")
    experts = columns * members // 2
    group = members // 2
    slot_cap = 5 * rows_here // (2 * experts)
    slots = experts * slot_cap
    half = width // LANES // 2
    assert group == 4

    def shift(even, odd):
        return [(i, (i + (odd if i % 2 else even)) % members) for i in range(members)]

    out_hops = (shift(-1, 1), shift(2, -2), shift(-3, 3))
    back_hops = tuple([(b, a) for a, b in hop] for hop in out_hops)
    swap = [(i, i ^ 1) for i in range(members)]

    def swapped(value):
        return lax.ppermute(value, "fsdp", swap)

    def spread(blocks, hops):
        return [blocks[0]] + [lax.ppermute(b, "fsdp", hop) for b, hop in zip(blocks[1:], hops)]

    def across(box):
        boxes = box.reshape(columns, group * slot_cap, half, LANES)
        return lax.all_to_all(boxes, "expert", split_axis=0, concat_axis=0, tiled=True).reshape(box.shape)

    block_shape = (columns * slot_cap, half, LANES)

    def split(box):
        parts = box.reshape(columns, group, slot_cap, half, LANES)
        return [parts[:, m].reshape(block_shape) for m in range(group)]

    def join(blocks):
        parts = [b.reshape(columns, 1, slot_cap, half, LANES) for b in blocks]
        return jnp.concatenate(parts, axis=1).reshape(slots, half, LANES)

    def add_halves(own, other):
        return (own.astype(jnp.float32) + other.astype(jnp.float32)).astype(jnp.bfloat16)

    here = lax.axis_index("fsdp")
    odd = here % 2
    depth = width // 2
    their_context = swapped(context)
    tokens_of = lambda h: lax.dynamic_slice_in_dim(tokens, h * depth, depth, axis=1)
    their_tokens = swapped(tokens_of(1 - odd))
    pieces = jnp.stack([out_proj[:, :depth], out_proj[:, depth:]])
    pieces = jnp.broadcast_to(pieces[None], (group,) + pieces.shape).reshape(members, -1, depth)
    pieces = lax.all_to_all(pieces, "fsdp", split_axis=0, concat_axis=0, tiled=True)
    proj = lax.all_gather(pieces.reshape(-1, depth), "expert", axis=0, tiled=True)

    def residual(tokens_part, context_rows):
        attended = jnp.dot(context_rows, proj, preferred_element_type=jnp.float32)
        return (tokens_part.astype(jnp.float32) + attended).astype(jnp.bfloat16)

    flat_ids, places = slot_places(expert_ids, experts)
    away = (flat_ids % group - here // 2) % group
    message = jnp.where(away == 0, 0, jnp.where(away == 2, 3, jnp.where((away == 1) == (odd == 0), 2, 1)))
    column = flat_ids // group
    by_column = ((column * group + message) * slot_cap + places).astype(jnp.int32)
    by_message = ((message * columns + column) * slot_cap + places).astype(jnp.int32)

    other = swapped(residual(their_tokens, their_context))
    mine = residual(tokens_of(odd), context)
    box_a, box_b, kept, gates = front(
        by_column,
        by_message,
        odd.astype(jnp.int32).reshape(1),
        mine,
        other,
        norm_gain.reshape(1, width),
        router,
        expert_ids,
        slots,
    )

    over_a = across(box_a)
    near_b = spread(list(box_b.reshape((group,) + block_shape)), out_hops)
    near_b = across(join(near_b))
    near_a = spread(split(over_a), out_hops)
    far_a = [swapped(b) for b in near_a]
    far_b = swapped(near_b)

    gate_up = experts_first(near_a + far_a, w_gate_up)
    hidden, own_a, other_a = experts_second((near_b, far_b), w_gate_up, w_down, gate_up, columns, group)
    sum_a = add_halves(own_a, swapped(other_a))
    made_b = experts_third(hidden, w_down, near_a + far_a)
    sum_b = {m: add_halves(made_b[m], swapped(made_b[group + m])) for m in (3, 2, 1, 0)}
    sum_a = across(sum_a)
    sum_b = join(spread([sum_b[m] for m in range(group)], back_hops))
    done_b = across(sum_b)
    done_a = jnp.concatenate(spread(split(sum_a), back_hops), axis=0)
    return back(by_message, by_column, gates.reshape(-1), done_a, done_b, kept)


def solution(mesh):
    rows = P(("sweep", "expert", "fsdp"), None)
    return jax.shard_map(
        on_device,
        mesh=mesh,
        in_specs=(
            rows,
            rows,
            rows,
            P("sweep"),
            P("sweep", None),
            rows,
            P(("sweep", "expert", "fsdp"), None, None, None),
            P(("sweep", "expert", "fsdp"), None, None),
        ),
        out_specs=rows,
        check_vma=False,
    )
```

```python
import functools

import jax
import jax.numpy as jnp
from jax import lax
from jax.experimental import pallas as pl
from jax.experimental.pallas import tpu as pltpu
from jax.sharding import PartitionSpec as P


eps_norm = 1e-05
LANES = 128

VMEM = pltpu.VMEM
SMEM = pltpu.SMEM


def whole(space):
    return pl.BlockSpec(memory_space=space)


def slot_places(expert_ids, experts):
    flat_ids = expert_ids.reshape(-1)
    onehot = (flat_ids[:, None] == jnp.arange(experts, dtype=jnp.int32)[None, :]).astype(jnp.int32)
    before = jnp.cumsum(onehot, axis=0) - onehot
    places = jnp.sum(before * onehot, axis=1)
    return (flat_ids, places)


def project_kernel(offsets, position, context, tokens, *refs):
    blocks, out = refs[:-1], refs[-1]
    count = context.shape[1] // blocks[0].shape[0] // 2
    row, core = position[0] // 2, position[0] % 2
    total = jnp.zeros(out.shape, jnp.float32)
    for (away, twin), block in zip(offsets, blocks):
        depth = block.shape[0]
        place = (lax.rem(row + away + count, count) * 2 + (core + twin) % 2) * depth
        part = context[:, pl.ds(pl.multiple_of(place, depth), depth)]
        total = total + jnp.dot(part, block[...], preferred_element_type=jnp.float32)
    out[...] = (tokens[...].astype(jnp.float32) + total).astype(jnp.bfloat16)


def project(offsets, position, context, tokens, blocks):
    return pl.pallas_call(
        functools.partial(project_kernel, offsets),
        in_specs=[whole(SMEM)] + [whole(VMEM)] * (2 + len(blocks)),
        out_specs=whole(VMEM),
        out_shape=jax.ShapeDtypeStruct(tokens.shape, jnp.bfloat16),
        cost_estimate=pl.CostEstimate(
            flops=2 * tokens.size * context.shape[1], bytes_accessed=2 * tokens.size, transcendentals=0
        ),
    )(position, context, tokens, *blocks)


def front_kernel(index_a, index_b, odd, mine, other, gain, router, ids, box_a, box_b, kept, gates, tiles):
    rows, depth = mine.shape
    chunks = 2 * depth // LANES
    half = chunks // 2
    swapped = odd[0] == 1
    own, got = mine[...].astype(jnp.float32), other[...].astype(jnp.float32)
    parts = (jnp.where(swapped, got, own), jnp.where(swapped, own, got))
    squares = sum(jnp.sum(p * p, axis=1, keepdims=True) for p in parts)
    inv_rms = lax.rsqrt(squares / (2 * depth) + eps_norm)
    for c in range(chunks):
        lane = c % half * LANES
        tiles[pl.ds(c, rows, stride=chunks), :] = parts[c // half][:, lane : lane + LANES]
    kept[...] = tiles[...].reshape(rows, chunks, LANES).astype(jnp.bfloat16)
    normed = [
        (p * inv_rms * gain[:, h * depth : (h + 1) * depth]).astype(jnp.bfloat16) for h, p in enumerate(parts)
    ]
    logits = sum(
        jnp.dot(p, router[h * depth : (h + 1) * depth, :], preferred_element_type=jnp.float32)
        for h, p in enumerate(normed)
    )
    lanes = lax.broadcasted_iota(jnp.int32, logits.shape, 1)
    scores = []
    for k in range(2):
        hit = lanes == ids[:, k : k + 1]
        picked = jnp.sum(jnp.where(hit, logits, 0.0), axis=1, keepdims=True)
        scores.append(jax.nn.sigmoid(picked))
    total = scores[0] + scores[1]
    gates[:, 0:1] = scores[0] / total
    gates[:, 1:2] = scores[1] / total
    wider = [p.astype(jnp.float32) for p in normed]
    for c in range(chunks):
        lane = c % half * LANES
        tiles[pl.ds(c, rows, stride=chunks), :] = wider[c // half][:, lane : lane + LANES]
    box_a[...] = jnp.zeros_like(box_a)
    box_b[...] = jnp.zeros_like(box_b)

    def place(t, carry):
        start = pl.multiple_of(t * chunks, chunks)
        first = tiles[pl.ds(start, half), :].astype(jnp.bfloat16)
        second = tiles[pl.ds(start + half, half), :].astype(jnp.bfloat16)
        for k in range(2):
            box_a[index_a[2 * t + k]] = first
            box_b[index_b[2 * t + k]] = second
        return carry

    lax.fori_loop(0, rows, place, 0, unroll=4)


def front(index_a, index_b, odd, mine, other, gain, router, ids, slots):
    rows, depth = mine.shape
    half = depth // LANES
    box = jax.ShapeDtypeStruct((slots, half, LANES), jnp.bfloat16)
    return pl.pallas_call(
        front_kernel,
        in_specs=[whole(SMEM)] * 3 + [whole(VMEM)] * 5,
        out_specs=[whole(VMEM)] * 4,
        out_shape=[
            box,
            box,
            jax.ShapeDtypeStruct((rows, 2 * half, LANES), jnp.bfloat16),
            jax.ShapeDtypeStruct((rows, 2), jnp.float32),
        ],
        scratch_shapes=[VMEM((rows * 2 * half, LANES), jnp.float32)],
        cost_estimate=pl.CostEstimate(flops=1 << 24, bytes_accessed=1 << 23, transcendentals=0),
    )(index_a, index_b, odd, mine, other, gain, router, ids)


def fill_blocks(blocks, lhs, tiles):
    for b, block in enumerate(blocks):
        rows, chunks, _ = block.shape
        tiles[pl.ds(b * rows * chunks, rows * chunks), :] = block[...].astype(jnp.float32).reshape(rows * chunks, LANES)
    unpack(lhs, tiles, chunks)


def fill_boxes(boxes, lhs, tiles, columns, group):
    rows, chunks, _ = boxes[0].shape
    cap = rows // (columns * group)
    for b, box in enumerate(boxes):
        for col in range(columns):
            for m in range(group):
                source = (col * group + m) * cap
                target = b * rows + (m * columns + col) * cap
                piece = box[source : source + cap].astype(jnp.float32)
                tiles[target * chunks : (target + cap) * chunks, :] = piece.reshape(cap * chunks, LANES)
    unpack(lhs, tiles, chunks)


def unpack(lhs, tiles, chunks):
    rows = lhs.shape[0]
    for c in range(chunks):
        lhs[:, c * LANES : (c + 1) * LANES] = tiles[pl.ds(c, rows, stride=chunks), :].astype(jnp.bfloat16)


def pack(value, tiles, chunks):
    rows = value.shape[0]
    rounded = value.astype(jnp.bfloat16).astype(jnp.float32)
    for c in range(chunks):
        tiles[pl.ds(c, rows, stride=chunks), :] = rounded[:, c * LANES : (c + 1) * LANES]


def empty_blocks(blocks, tiles):
    for b, block in enumerate(blocks):
        rows, chunks, _ = block.shape
        piece = tiles[b * rows * chunks : (b + 1) * rows * chunks, :]
        block[...] = piece.reshape(rows, chunks, LANES).astype(jnp.bfloat16)


def empty_boxes(boxes, tiles, columns, group):
    rows, chunks, _ = boxes[0].shape
    cap = rows // (columns * group)
    for b, box in enumerate(boxes):
        for col in range(columns):
            for m in range(group):
                target = (col * group + m) * cap
                source = b * rows + (m * columns + col) * cap
                piece = tiles[source * chunks : (source + cap) * chunks, :]
                box[target : target + cap] = piece.reshape(cap, chunks, LANES).astype(jnp.bfloat16)


def dot_t(lhs, rhs):
    return lax.dot_general(lhs, rhs, (((1,), (1,)), ((), ())), preferred_element_type=jnp.float32)


def gate_first_kernel(*refs):
    blocks, (weight, out, lhs, tiles) = refs[:8], refs[8:]
    fill_blocks(blocks, lhs, tiles)
    for k in range(2):
        out[k] = dot_t(lhs[...], weight[0, k])


def gate_second_kernel(columns, group, *refs):
    boxes, (weight, down, gate_up, hidden), outs, (lhs, tiles) = refs[:2], refs[2:6], refs[6:8], refs[8:]
    fill_boxes(boxes, lhs, tiles, columns, group)
    gate = gate_up[0] + dot_t(lhs[...], weight[0, 0])
    up = gate_up[1] + dot_t(lhs[...], weight[0, 1])
    hidden[...] = (gate / (1.0 + jnp.exp(-gate)) * up).astype(jnp.bfloat16)
    pack(jnp.dot(hidden[...], down[0], preferred_element_type=jnp.float32), tiles, outs[0].shape[1])
    empty_boxes(outs, tiles, columns, group)


def down_second_kernel(hidden, down, *refs):
    outs, (tiles,) = refs[:-1], refs[-1:]
    pack(jnp.dot(hidden[...], down[0], preferred_element_type=jnp.float32), tiles, outs[0].shape[1])
    empty_blocks(outs, tiles)


def experts_first(blocks, w_gate_up):
    rows, chunks, _ = blocks[0].shape
    total, depth, units = rows * len(blocks), chunks * LANES, w_gate_up.shape[2]
    return pl.pallas_call(
        gate_first_kernel,
        grid=(1,),
        in_specs=[whole(VMEM)] * 8 + [pl.BlockSpec((1, 2, units, depth), lambda n: (0, 0, 0, 0))],
        out_specs=pl.BlockSpec((2, total, units), lambda n: (0, 0, 0)),
        out_shape=jax.ShapeDtypeStruct((2, total, units), jnp.float32),
        scratch_shapes=[VMEM((total, depth), jnp.bfloat16), VMEM((total * chunks, LANES), jnp.float32)],
        cost_estimate=pl.CostEstimate(
            flops=4 * total * depth * units, bytes_accessed=4 * units * depth, transcendentals=0
        ),
    )(*blocks, w_gate_up)


def experts_second(boxes, w_gate_up, w_down, gate_up, columns, group):
    rows, chunks, _ = boxes[0].shape
    total, depth, units = rows * len(boxes), chunks * LANES, w_gate_up.shape[2]
    box = jax.ShapeDtypeStruct(boxes[0].shape, jnp.bfloat16)
    return pl.pallas_call(
        functools.partial(gate_second_kernel, columns, group),
        grid=(1,),
        in_specs=[whole(VMEM)] * 2
        + [
            pl.BlockSpec((1, 2, units, depth), lambda n: (0, 0, 0, 1)),
            pl.BlockSpec((1, units, depth), lambda n: (0, 0, 0)),
            whole(VMEM),
        ],
        out_specs=[whole(VMEM)] * 3,
        out_shape=[jax.ShapeDtypeStruct((total, units), jnp.bfloat16), box, box],
        scratch_shapes=[VMEM((total, depth), jnp.bfloat16), VMEM((total * chunks, LANES), jnp.float32)],
        cost_estimate=pl.CostEstimate(
            flops=6 * total * depth * units, bytes_accessed=6 * units * depth, transcendentals=total * units
        ),
    )(*boxes, w_gate_up, w_down, gate_up)


def experts_third(hidden, w_down, like):
    total, units = hidden.shape
    chunks = like[0].shape[1]
    depth = chunks * LANES
    return pl.pallas_call(
        down_second_kernel,
        grid=(1,),
        in_specs=[whole(VMEM), pl.BlockSpec((1, units, depth), lambda n: (0, 0, 1))],
        out_specs=[whole(VMEM)] * len(like),
        out_shape=[jax.ShapeDtypeStruct(b.shape, b.dtype) for b in like],
        scratch_shapes=[VMEM((total * chunks, LANES), jnp.float32)],
        cost_estimate=pl.CostEstimate(
            flops=2 * total * depth * units, bytes_accessed=2 * units * depth, transcendentals=0
        ),
    )(hidden, w_down)


def back_kernel(index_a, index_b, gates, from_a, from_b, kept, out, tiles):
    rows, chunks, _ = kept.shape
    half = chunks // 2

    def token(t, carry):
        start = pl.multiple_of(t * chunks, chunks)
        value = kept[t].astype(jnp.float32)
        first, second = value[:half], value[half:]
        for k in range(2):
            gate = gates[2 * t + k]
            first = first + gate * from_a[index_a[2 * t + k]].astype(jnp.float32)
            second = second + gate * from_b[index_b[2 * t + k]].astype(jnp.float32)
        tiles[pl.ds(start, half), :] = first
        tiles[pl.ds(start + half, half), :] = second
        return carry

    lax.fori_loop(0, rows, token, 0, unroll=4)
    for c in range(chunks):
        out[:, c * LANES : (c + 1) * LANES] = tiles[pl.ds(c, rows, stride=chunks), :].astype(jnp.bfloat16)


def back(index_a, index_b, gates, from_a, from_b, kept):
    rows, chunks, _ = kept.shape
    return pl.pallas_call(
        back_kernel,
        in_specs=[whole(SMEM)] * 3 + [whole(VMEM)] * 3,
        out_specs=whole(VMEM),
        out_shape=jax.ShapeDtypeStruct((rows, chunks * LANES), jnp.bfloat16),
        scratch_shapes=[VMEM((rows * chunks, LANES), jnp.float32)],
        cost_estimate=pl.CostEstimate(flops=1 << 20, bytes_accessed=1 << 22, transcendentals=0),
    )(index_a, index_b, gates, from_a, from_b, kept)


def on_device(tokens, context, out_proj, norm_gain, router, expert_ids, w_gate_up, w_down):
    rows_here, width = tokens.shape
    columns = lax.axis_size("expert")
    members = lax.axis_size("fsdp")
    experts = columns * members // 2
    group = members // 2
    slot_cap = 5 * rows_here // (2 * experts)
    slots = experts * slot_cap
    half = width // LANES // 2
    assert group == 4

    def shift(even, odd):
        return [(i, (i + (odd if i % 2 else even)) % members) for i in range(members)]

    out_hops = (shift(-1, 1), shift(2, -2), shift(-3, 3))
    back_hops = tuple([(b, a) for a, b in hop] for hop in out_hops)
    swap = [(i, i ^ 1) for i in range(members)]

    def swapped(value):
        return lax.ppermute(value, "fsdp", swap)

    def spread(blocks, hops):
        return [blocks[0]] + [lax.ppermute(b, "fsdp", hop) for b, hop in zip(blocks[1:], hops)]

    def across(box):
        boxes = box.reshape(columns, group * slot_cap, half, LANES)
        return lax.all_to_all(boxes, "expert", split_axis=0, concat_axis=0, tiled=True).reshape(box.shape)

    block_shape = (columns * slot_cap, half, LANES)

    def split(box):
        parts = box.reshape(columns, group, slot_cap, half, LANES)
        return [parts[:, m].reshape(block_shape) for m in range(group)]

    def join(blocks):
        parts = [b.reshape(columns, 1, slot_cap, half, LANES) for b in blocks]
        return jnp.concatenate(parts, axis=1).reshape(slots, half, LANES)

    def add_halves(own, other):
        return (own.astype(jnp.float32) + other.astype(jnp.float32)).astype(jnp.bfloat16)

    here = lax.axis_index("fsdp")
    odd = here % 2
    depth = width // 2
    their_context = swapped(context)
    tokens_of = lambda h: lax.dynamic_slice_in_dim(tokens, h * depth, depth, axis=1)
    their_tokens = swapped(tokens_of(1 - odd))
    pieces = jnp.stack([out_proj[:, :depth], out_proj[:, depth:]])
    pieces = jnp.broadcast_to(pieces[None], (group,) + pieces.shape).reshape(members, -1, depth)
    pieces = lax.all_to_all(pieces, "fsdp", split_axis=0, concat_axis=0, tiled=True)
    block = pieces.reshape(-1, depth)
    hop = lambda value, by: lax.ppermute(value, "expert", [(i, (i + by) % columns) for i in range(columns)])
    twin = lambda value: lax.ppermute(value, "expert", [(i, i ^ 1) for i in range(columns)])
    upward, downward, blocks = [block], [block], {0: block}
    reach = columns // 4
    for k in range(1, reach):
        upward.append(hop(upward[-1], 2))
        downward.append(hop(downward[-1], -2))
        blocks[-k], blocks[k] = upward[k], downward[k]
    cut = block.shape[0] // 2
    ends = [hop(upward[-1][:cut], 2), hop(downward[-1][cut:], -2)]
    blocks[reach] = jnp.concatenate(ends, axis=0)
    twins = {k: twin(v) for k, v in blocks.items()}
    offsets = tuple((k, t) for t in range(2) for k in blocks)
    held = list(blocks.values()) + list(twins.values())
    position = lax.axis_index("expert").astype(jnp.int32).reshape(1)

    flat_ids, places = slot_places(expert_ids, experts)
    away = (flat_ids % group - here // 2) % group
    message = jnp.where(away == 0, 0, jnp.where(away == 2, 3, jnp.where((away == 1) == (odd == 0), 2, 1)))
    column = flat_ids // group
    by_column = ((column * group + message) * slot_cap + places).astype(jnp.int32)
    by_message = ((message * columns + column) * slot_cap + places).astype(jnp.int32)

    other = swapped(project(offsets, position, their_context, their_tokens, held))
    mine = project(offsets, position, context, tokens_of(odd), held)
    box_a, box_b, kept, gates = front(
        by_column,
        by_message,
        odd.astype(jnp.int32).reshape(1),
        mine,
        other,
        norm_gain.reshape(1, width),
        router,
        expert_ids,
        slots,
    )

    over_a = across(box_a)
    near_b = spread(list(box_b.reshape((group,) + block_shape)), out_hops)
    near_b = across(join(near_b))
    near_a = spread(split(over_a), out_hops)
    far_a = [swapped(b) for b in near_a]
    far_b = swapped(near_b)

    gate_up = experts_first(near_a + far_a, w_gate_up)
    hidden, own_a, other_a = experts_second((near_b, far_b), w_gate_up, w_down, gate_up, columns, group)
    sum_a = add_halves(own_a, swapped(other_a))
    made_b = experts_third(hidden, w_down, near_a + far_a)
    sum_b = {}
    for m in (1, 2, 3, 0):
        sum_b[m] = add_halves(made_b[m], swapped(made_b[group + m]))
    sum_a = across(sum_a)
    sum_b = join(spread([sum_b[m] for m in range(group)], back_hops))
    done_b = across(sum_b)
    done_a = jnp.concatenate(spread(split(sum_a), back_hops), axis=0)
    return back(by_message, by_column, gates.reshape(-1), done_a, done_b, kept)


def solution(mesh):
    rows = P(("sweep", "expert", "fsdp"), None)
    return jax.shard_map(
        on_device,
        mesh=mesh,
        in_specs=(
            rows,
            rows,
            rows,
            P("sweep"),
            P("sweep", None),
            rows,
            P(("sweep", "expert", "fsdp"), None, None, None),
            P(("sweep", "expert", "fsdp"), None, None),
        ),
        out_specs=rows,
        check_vma=False,
    )
```

```python
import functools

import jax
import jax.numpy as jnp
from jax import lax
from jax.experimental import pallas as pl
from jax.experimental.pallas import tpu as pltpu
from jax.sharding import PartitionSpec as P


eps_norm = 1e-05
LANES = 128
LIMIT = 10 << 20

VMEM = pltpu.VMEM
SMEM = pltpu.SMEM


def whole(space):
    return pl.BlockSpec(memory_space=space)


def slot_places(expert_ids, experts):
    flat_ids = expert_ids.reshape(-1)
    onehot = (flat_ids[:, None] == jnp.arange(experts, dtype=jnp.int32)[None, :]).astype(jnp.int32)
    before = jnp.cumsum(onehot, axis=0) - onehot
    places = jnp.sum(before * onehot, axis=1)
    return (flat_ids, places)


def project_kernel(offsets, position, context, tokens, *refs):
    blocks, out = refs[:-1], refs[-1]
    count = len(offsets) // 2
    row, core = position[0] // 2, position[0] % 2
    depth = context.shape[1] // len(offsets)
    parts = []
    for away, twin in offsets:
        place = (lax.rem(row + away + count, count) * 2 + (core + twin) % 2) * depth
        parts.append(context[:, pl.ds(pl.multiple_of(place, depth), depth)])
    rows = jnp.concatenate(parts, axis=1)
    step = out.shape[1] // 4

    def piece(n, carry):
        lanes = pl.ds(pl.multiple_of(n * step, step), step)
        total = jnp.dot(
            rows,
            jnp.concatenate([block[:, lanes] for block in blocks], axis=0),
            preferred_element_type=jnp.float32,
        )
        out[:, lanes] = (tokens[:, lanes].astype(jnp.float32) + total).astype(jnp.bfloat16)
        return carry

    lax.fori_loop(0, 4, piece, 0)


def project(offsets, position, context, tokens, blocks):
    return pl.pallas_call(
        functools.partial(project_kernel, offsets),
        in_specs=[whole(SMEM)] + [whole(VMEM)] * (2 + len(blocks)),
        out_specs=whole(VMEM),
        out_shape=jax.ShapeDtypeStruct(tokens.shape, jnp.bfloat16),
        compiler_params=pltpu.CompilerParams(vmem_limit_bytes=LIMIT),
        cost_estimate=pl.CostEstimate(
            flops=2 * tokens.size * context.shape[1], bytes_accessed=2 * tokens.size, transcendentals=0
        ),
    )(position, context, tokens, *blocks)


def front_kernel(index, odd, mine, other, gain, router, ids, box_a, *refs):
    boxes_b, (kept, gates, tiles, box) = refs[:-4], refs[-4:]
    rows, depth = mine.shape
    chunks = 2 * depth // LANES
    half = chunks // 2
    swapped = odd[0] == 1
    own, got = mine[...].astype(jnp.float32), other[...].astype(jnp.float32)
    parts = (jnp.where(swapped, got, own), jnp.where(swapped, own, got))
    squares = sum(jnp.sum(p * p, axis=1, keepdims=True) for p in parts)
    inv_rms = lax.rsqrt(squares / (2 * depth) + eps_norm)
    for c in range(chunks):
        lane = c % half * LANES
        tiles[pl.ds(c, rows, stride=chunks), :] = parts[c // half][:, lane : lane + LANES]
    kept[...] = tiles[...].reshape(rows, chunks, LANES).astype(jnp.bfloat16)
    normed = [
        (p * inv_rms * gain[:, h * depth : (h + 1) * depth]).astype(jnp.bfloat16) for h, p in enumerate(parts)
    ]
    logits = sum(
        jnp.dot(p, router[h * depth : (h + 1) * depth, :], preferred_element_type=jnp.float32)
        for h, p in enumerate(normed)
    )
    lanes = lax.broadcasted_iota(jnp.int32, logits.shape, 1)
    scores = []
    for k in range(2):
        hit = lanes == ids[:, k : k + 1]
        picked = jnp.sum(jnp.where(hit, logits, 0.0), axis=1, keepdims=True)
        scores.append(jax.nn.sigmoid(picked))
    total = scores[0] + scores[1]
    gates[:, 0:1] = scores[0] / total
    gates[:, 1:2] = scores[1] / total
    wider = [p.astype(jnp.float32) for p in normed]
    for c in range(chunks):
        lane = c % half * LANES
        tiles[pl.ds(c, rows, stride=chunks), :] = wider[c // half][:, lane : lane + LANES]
    box[...] = jnp.zeros_like(box)

    def place(t, carry):
        start = pl.multiple_of(t * chunks, chunks)
        line = tiles[pl.ds(start, chunks), :].astype(jnp.bfloat16)
        box[index[2 * t]] = line
        box[index[2 * t + 1]] = line
        return carry

    lax.fori_loop(0, rows, place, 0, unroll=4)
    start = box_a.shape[0]
    box_a[...] = box[:start]
    for part in boxes_b:
        part[...] = box[start : start + part.shape[0]]
        start += part.shape[0]


def front(index, odd, mine, other, gain, router, ids, sizes):
    rows, depth = mine.shape
    chunks = 2 * depth // LANES
    box = lambda n: jax.ShapeDtypeStruct((n, chunks, LANES), jnp.bfloat16)
    got = pl.pallas_call(
        front_kernel,
        in_specs=[whole(SMEM)] * 2 + [whole(VMEM)] * 5,
        out_specs=[whole(VMEM)] * (len(sizes) + 2),
        out_shape=[box(n) for n in sizes] + [box(rows), jax.ShapeDtypeStruct((rows, 2), jnp.float32)],
        scratch_shapes=[VMEM((rows * chunks, LANES), jnp.float32), VMEM((sum(sizes), chunks, LANES), jnp.bfloat16)],
        compiler_params=pltpu.CompilerParams(vmem_limit_bytes=LIMIT),
        cost_estimate=pl.CostEstimate(flops=1 << 24, bytes_accessed=1 << 23, transcendentals=0),
    )(index, odd, mine, other, gain, router, ids)
    return got[0], got[1:-2], got[-2], got[-1]


def dot_t(lhs, rhs):
    return lax.dot_general(lhs, rhs, (((1,), (1,)), ((), ())), preferred_element_type=jnp.float32)


def experts_kernel(count, turns, moves, *refs):
    ins, (gate_up, down), outs = refs[:count], refs[count : count + 2], refs[count + 2 : -4]
    lhs, tiles, both, hidden = refs[-4:]
    rows, wide = lhs.shape
    chunks = wide // LANES
    group = 16
    start = 0
    for block in ins:

        def widen(r, carry, block=block, start=start):
            piece = block[pl.ds(pl.multiple_of(r * group, group), group)].astype(jnp.float32)
            tiles[pl.ds(pl.multiple_of((start + r * group) * chunks, group * chunks), group * chunks), :] = (
                piece.reshape(group * chunks, LANES)
            )
            return carry

        lax.fori_loop(0, block.shape[0] // group, widen, 0)
        start += block.shape[0]

    def spread_lanes(r, carry):
        for c in range(chunks):
            piece = tiles[pl.ds(r * group * chunks + c, group, stride=chunks), :]
            lhs[pl.ds(pl.multiple_of(r * group, group), group), c * LANES : (c + 1) * LANES] = piece.astype(jnp.bfloat16)
        return carry

    lax.fori_loop(0, rows // group, spread_lanes, 0)

    def project_up(k, carry):
        both[k] = dot_t(gate_up[0, k], lhs[...])
        return carry

    lax.fori_loop(0, 2, project_up, 0)
    gate = both[0]
    hidden[...] = (gate / (1.0 + jnp.exp(-gate)) * both[1]).T.astype(jnp.bfloat16)
    step = wide // 4

    def project_down(n, carry):
        part = down[0, :, pl.ds(pl.multiple_of(n * step, step), step)]
        made = jnp.dot(hidden[...], part, preferred_element_type=jnp.float32)
        for c in range(step // LANES):
            tiles[pl.ds(n * (step // LANES) + c, rows, stride=chunks), :] = made[:, c * LANES : (c + 1) * LANES]
        return carry

    lax.fori_loop(0, 4, project_down, 0)

    def settle(turn, carry):
        for out, target, target_step, source, source_step, size in moves:
            place = pl.multiple_of((source + turn * source_step) * chunks, chunks)
            piece = tiles[pl.ds(place, size * chunks), :].reshape(size, chunks, LANES)
            outs[out][pl.ds(target + turn * target_step, size)] = piece.astype(jnp.bfloat16)
        return carry

    lax.fori_loop(0, turns, settle, 0)


def run_experts(ins, w_gate_up, w_down, turns, moves, sizes):
    chunks = ins[0].shape[1]
    rows, wide, units = sum(b.shape[0] for b in ins), chunks * LANES, w_down.shape[1]
    return pl.pallas_call(
        functools.partial(experts_kernel, len(ins), turns, moves),
        in_specs=[whole(VMEM)] * (len(ins) + 2),
        out_specs=[whole(VMEM)] * len(sizes),
        out_shape=[jax.ShapeDtypeStruct((n, chunks, LANES), jnp.bfloat16) for n in sizes],
        scratch_shapes=[
            VMEM((rows, wide), jnp.bfloat16),
            VMEM((rows * chunks, LANES), jnp.float32),
            VMEM((2, units, rows), jnp.float32),
            VMEM((rows, units), jnp.bfloat16),
        ],
        compiler_params=pltpu.CompilerParams(vmem_limit_bytes=2 * LIMIT),
        cost_estimate=pl.CostEstimate(
            flops=6 * rows * wide * units, bytes_accessed=6 * units * wide, transcendentals=rows * units
        ),
    )(*ins, w_gate_up, w_down)


def back_kernel(index, gates, *refs):
    boxes, (kept, out, tiles, box) = refs[:-4], refs[-4:]
    rows, chunks, _ = kept.shape
    start = 0
    for part in boxes:
        box[start : start + part.shape[0]] = part[...]
        start += part.shape[0]

    def token(t, carry):
        value = kept[t].astype(jnp.float32)
        for k in range(2):
            value = value + gates[2 * t + k] * box[index[2 * t + k]].astype(jnp.float32)
        tiles[pl.ds(pl.multiple_of(t * chunks, chunks), chunks), :] = value
        return carry

    lax.fori_loop(0, rows, token, 0, unroll=4)
    for c in range(chunks):
        out[:, c * LANES : (c + 1) * LANES] = tiles[pl.ds(c, rows, stride=chunks), :].astype(jnp.bfloat16)


def back(index, gates, boxes, kept):
    rows, chunks, _ = kept.shape
    total = sum(b.shape[0] for b in boxes)
    return pl.pallas_call(
        back_kernel,
        in_specs=[whole(SMEM)] * 2 + [whole(VMEM)] * (len(boxes) + 1),
        out_specs=whole(VMEM),
        out_shape=jax.ShapeDtypeStruct((rows, chunks * LANES), jnp.bfloat16),
        scratch_shapes=[VMEM((rows * chunks, LANES), jnp.float32), VMEM((total, chunks, LANES), jnp.bfloat16)],
        compiler_params=pltpu.CompilerParams(vmem_limit_bytes=LIMIT),
        cost_estimate=pl.CostEstimate(flops=1 << 20, bytes_accessed=1 << 22, transcendentals=0),
    )(index, gates, *boxes, kept)


def on_device(tokens, context, out_proj, norm_gain, router, expert_ids, w_gate_up, w_down):
    rows_here, width = tokens.shape
    columns = lax.axis_size("expert")
    members = lax.axis_size("fsdp")
    experts = columns * members // 2
    group = members // 2
    slot_cap = 5 * rows_here // (2 * experts)
    chunks = width // LANES
    assert group == 4

    def shift(even, odd):
        return [(i, (i + (odd if i % 2 else even)) % members) for i in range(members)]

    out_hops = (shift(-1, 1), shift(2, -2), shift(-3, 3))
    back_hops = tuple([(b, a) for a, b in hop] for hop in out_hops)
    swap = [(i, i ^ 1) for i in range(members)]

    def swapped(value):
        return lax.ppermute(value, "fsdp", swap)

    def spread(blocks, hops):
        return [blocks[0]] + [lax.ppermute(b, "fsdp", hop) for b, hop in zip(blocks[1:], hops)]

    def across(box):
        boxes = box.reshape(columns, -1, chunks, LANES)
        return lax.all_to_all(boxes, "expert", split_axis=0, concat_axis=0, tiled=True).reshape(box.shape)

    def split(box):
        parts = box.reshape(columns, group, -1, chunks, LANES)
        return [parts[:, m].reshape(-1, chunks, LANES) for m in range(group)]

    def join(blocks):
        parts = [b.reshape(columns, 1, -1, chunks, LANES) for b in blocks]
        return jnp.concatenate(parts, axis=1).reshape(-1, chunks, LANES)

    def add_halves(own, other):
        return (own.astype(jnp.float32) + other.astype(jnp.float32)).astype(jnp.bfloat16)

    here = lax.axis_index("fsdp")
    odd = here % 2
    depth = width // 2
    tokens_of = lambda h: lax.dynamic_slice_in_dim(tokens, h * depth, depth, axis=1)
    their_context = swapped(context)
    their_tokens = swapped(tokens_of(1 - odd))
    pieces = jnp.stack([out_proj[:, :depth], out_proj[:, depth:]])
    pieces = jnp.broadcast_to(pieces[None], (group,) + pieces.shape).reshape(members, -1, depth)
    pieces = lax.all_to_all(pieces, "fsdp", split_axis=0, concat_axis=0, tiled=True)
    block = pieces.reshape(-1, depth)
    hop = lambda value, by: lax.ppermute(value, "expert", [(i, (i + by) % columns) for i in range(columns)])
    twin = lambda value: lax.ppermute(value, "expert", [(i, i ^ 1) for i in range(columns)])
    upward, downward, held, offsets = [block], [block], [block], [(0, 0)]
    reach = columns // 4
    for k in range(1, reach):
        upward.append(hop(upward[-1], 2))
        downward.append(hop(downward[-1], -2))
        held.append(jnp.concatenate([upward[k], downward[k]], axis=0))
        offsets += [(-k, 0), (k, 0)]
    cut = block.shape[0] // 2
    ends = [hop(upward[-1][:cut], 2), hop(downward[-1][cut:], -2)]
    held.append(jnp.concatenate(ends, axis=0))
    offsets.append((reach, 0))
    held += [twin(v) for v in held]
    offsets = tuple(offsets + [(away, 1) for away, _ in offsets])
    position = lax.axis_index("expert").astype(jnp.int32).reshape(1)

    flat_ids, places = slot_places(expert_ids, experts)
    away = (flat_ids % group - here // 2) % group
    message = jnp.where(away == 0, 0, jnp.where(away == 2, 3, jnp.where((away == 1) == (odd == 0), 2, 1)))
    column = flat_ids // group
    cap_b = slot_cap // 2
    cap_a = slot_cap - cap_b
    lines = columns * group
    by_column = column * group + message
    by_message = message * columns + column
    early = places < cap_a
    first = lines * cap_a
    index_out = jnp.where(early, by_column * cap_a + places, first + by_message * cap_b + places - cap_a)
    index_in = jnp.where(early, by_message * cap_a + places, first + by_column * cap_b + places - cap_a)
    index_out, index_in = index_out.astype(jnp.int32), index_in.astype(jnp.int32)
    moves_a = tuple(
        (d, m * cap_a, group * cap_a, (d * group + m) * columns * cap_a, cap_a, cap_a)
        for d in range(2)
        for m in range(group)
    )
    moves_b = tuple(
        (2 * d + (m > 0), max(m - 1, 0) * columns * cap_b, cap_b, (d * lines + m) * cap_b, group * cap_b, cap_b)
        for d in range(2)
        for m in range(group)
    )

    other = swapped(project(offsets, position, their_context, their_tokens, held))
    mine = project(offsets, position, context, tokens_of(odd), held)
    sizes = [lines * cap_a] + [columns * cap_b] * group
    box_a, boxes_b, kept, gates = front(
        index_out,
        odd.astype(jnp.int32).reshape(1),
        mine,
        other,
        norm_gain.reshape(1, width),
        router,
        expert_ids,
        sizes,
    )

    over_a = across(box_a)
    near_b = spread(boxes_b, out_hops)
    near_b = across(join(near_b))
    near_a = spread(split(over_a), out_hops)
    far_a = [swapped(b) for b in near_a]
    far_b = swapped(near_b)

    own_a, other_a = run_experts(near_a + far_a, w_gate_up, w_down, columns, moves_a, [lines * cap_a] * 2)
    sum_a = add_halves(own_a, swapped(other_a))
    few = columns * cap_b
    made_b = run_experts([near_b, far_b], w_gate_up, w_down, columns, moves_b, [few, (group - 1) * few] * 2)
    going = add_halves(made_b[1], swapped(made_b[3]))
    staying = add_halves(made_b[0], swapped(made_b[2]))
    sum_b = [staying] + [going[m * few : (m + 1) * few] for m in range(group - 1)]
    sum_a = across(sum_a)
    sum_b = join(spread(sum_b, back_hops))
    done_b = across(sum_b)
    done_a = spread(split(sum_a), back_hops)
    return back(index_in, gates.reshape(-1), done_a + [done_b], kept)


def solution(mesh):
    rows = P(("sweep", "expert", "fsdp"), None)
    return jax.shard_map(
        on_device,
        mesh=mesh,
        in_specs=(
            rows,
            rows,
            rows,
            P("sweep"),
            P("sweep", None),
            rows,
            P(("sweep", "expert", "fsdp"), None, None, None),
            P(("sweep", "expert", "fsdp"), None, None),
        ),
        out_specs=rows,
        check_vma=False,
    )
```

```python
import functools

import jax
import jax.numpy as jnp
from jax import lax
from jax.experimental import pallas as pl
from jax.experimental.pallas import tpu as pltpu
from jax.sharding import PartitionSpec as P


eps_norm = 1e-05
LANES = 128
LIMIT = 10 << 20

VMEM = pltpu.VMEM
SMEM = pltpu.SMEM


def whole(space):
    return pl.BlockSpec(memory_space=space)


def slot_places(expert_ids, experts):
    flat_ids = expert_ids.reshape(-1)
    onehot = (flat_ids[:, None] == jnp.arange(experts, dtype=jnp.int32)[None, :]).astype(jnp.int32)
    before = jnp.cumsum(onehot, axis=0) - onehot
    places = jnp.sum(before * onehot, axis=1)
    return (flat_ids, places)


def project_kernel(offsets, position, context, tokens, *refs):
    blocks, out = refs[:-1], refs[-1]
    count = len(offsets) // 2
    row, core = position[0] // 2, position[0] % 2
    depth = context.shape[1] // len(offsets)
    parts = []
    for away, twin in offsets:
        place = (lax.rem(row + away + count, count) * 2 + (core + twin) % 2) * depth
        parts.append(context[:, pl.ds(pl.multiple_of(place, depth), depth)])
    rows = jnp.concatenate(parts, axis=1)
    step = out.shape[1] // 4

    def piece(n, carry):
        lanes = pl.ds(pl.multiple_of(n * step, step), step)
        total = jnp.dot(
            rows,
            jnp.concatenate([block[:, lanes] for block in blocks], axis=0),
            preferred_element_type=jnp.float32,
        )
        out[:, lanes] = (tokens[:, lanes].astype(jnp.float32) + total).astype(jnp.bfloat16)
        return carry

    lax.fori_loop(0, 4, piece, 0)


def project(offsets, position, context, tokens, blocks):
    return pl.pallas_call(
        functools.partial(project_kernel, offsets),
        in_specs=[whole(SMEM)] + [whole(VMEM)] * (2 + len(blocks)),
        out_specs=whole(VMEM),
        out_shape=jax.ShapeDtypeStruct(tokens.shape, jnp.bfloat16),
        compiler_params=pltpu.CompilerParams(vmem_limit_bytes=LIMIT),
        cost_estimate=pl.CostEstimate(
            flops=2 * tokens.size * context.shape[1], bytes_accessed=2 * tokens.size, transcendentals=0
        ),
    )(position, context, tokens, *blocks)


def front_kernel(index, odd, mine, other, gain, router, ids, box_a, *refs):
    boxes_b, (kept, gates, tiles, box) = refs[:-4], refs[-4:]
    rows, depth = mine.shape
    chunks = 2 * depth // LANES
    half = chunks // 2
    swapped = odd[0] == 1
    own, got = mine[...].astype(jnp.float32), other[...].astype(jnp.float32)
    parts = (jnp.where(swapped, got, own), jnp.where(swapped, own, got))
    squares = sum(jnp.sum(p * p, axis=1, keepdims=True) for p in parts)
    inv_rms = lax.rsqrt(squares / (2 * depth) + eps_norm)
    for c in range(chunks):
        lane = c % half * LANES
        tiles[pl.ds(c, rows, stride=chunks), :] = parts[c // half][:, lane : lane + LANES]
    kept[...] = tiles[...].reshape(rows, chunks, LANES).astype(jnp.bfloat16)
    normed = [
        (p * inv_rms * gain[:, h * depth : (h + 1) * depth]).astype(jnp.bfloat16) for h, p in enumerate(parts)
    ]
    logits = sum(
        jnp.dot(p, router[h * depth : (h + 1) * depth, :], preferred_element_type=jnp.float32)
        for h, p in enumerate(normed)
    )
    lanes = lax.broadcasted_iota(jnp.int32, logits.shape, 1)
    scores = []
    for k in range(2):
        hit = lanes == ids[:, k : k + 1]
        picked = jnp.sum(jnp.where(hit, logits, 0.0), axis=1, keepdims=True)
        scores.append(jax.nn.sigmoid(picked))
    total = scores[0] + scores[1]
    gates[:, 0:1] = scores[0] / total
    gates[:, 1:2] = scores[1] / total
    wider = [p.astype(jnp.float32) for p in normed]
    for c in range(chunks):
        lane = c % half * LANES
        tiles[pl.ds(c, rows, stride=chunks), :] = wider[c // half][:, lane : lane + LANES]
    box[...] = jnp.zeros_like(box)

    def place(t, carry):
        start = pl.multiple_of(t * chunks, chunks)
        line = tiles[pl.ds(start, chunks), :].astype(jnp.bfloat16)
        box[index[2 * t]] = line
        box[index[2 * t + 1]] = line
        return carry

    lax.fori_loop(0, rows, place, 0, unroll=4)
    start = box_a.shape[0]
    box_a[...] = box[:start]
    for part in boxes_b:
        part[...] = box[start : start + part.shape[0]]
        start += part.shape[0]


def front(index, odd, mine, other, gain, router, ids, sizes):
    rows, depth = mine.shape
    chunks = 2 * depth // LANES
    box = lambda n: jax.ShapeDtypeStruct((n, chunks, LANES), jnp.bfloat16)
    got = pl.pallas_call(
        front_kernel,
        in_specs=[whole(SMEM)] * 2 + [whole(VMEM)] * 5,
        out_specs=[whole(VMEM)] * (len(sizes) + 2),
        out_shape=[box(n) for n in sizes] + [box(rows), jax.ShapeDtypeStruct((rows, 2), jnp.float32)],
        scratch_shapes=[VMEM((rows * chunks, LANES), jnp.float32), VMEM((sum(sizes), chunks, LANES), jnp.bfloat16)],
        compiler_params=pltpu.CompilerParams(vmem_limit_bytes=LIMIT),
        cost_estimate=pl.CostEstimate(flops=1 << 24, bytes_accessed=1 << 23, transcendentals=0),
    )(index, odd, mine, other, gain, router, ids)
    return got[0], got[1:-2], got[-2], got[-1]


def dot_t(lhs, rhs):
    return lax.dot_general(lhs, rhs, (((1,), (1,)), ((), ())), preferred_element_type=jnp.float32)


def experts_kernel(count, turns, moves, *refs):
    ins, (gate_up_far, down_far), outs = refs[:count], refs[count : count + 2], refs[count + 2 : -7]
    lhs, tiles, both, hidden, gate_up, down, arrived = refs[-7:]

    def fetch(k):
        return pltpu.make_async_copy(gate_up_far.at[0, k], gate_up.at[k], arrived.at[k])

    fetch_down = pltpu.make_async_copy(down_far.at[0], down, arrived.at[2])
    fetch(0).start()
    fetch(1).start()
    fetch_down.start()
    rows, wide = lhs.shape
    chunks = wide // LANES
    group = 16
    start = 0
    for block in ins:

        def widen(r, carry, block=block, start=start):
            piece = block[pl.ds(pl.multiple_of(r * group, group), group)].astype(jnp.float32)
            tiles[pl.ds(pl.multiple_of((start + r * group) * chunks, group * chunks), group * chunks), :] = (
                piece.reshape(group * chunks, LANES)
            )
            return carry

        lax.fori_loop(0, block.shape[0] // group, widen, 0)
        start += block.shape[0]

    def spread_lanes(r, carry):
        for c in range(chunks):
            piece = tiles[pl.ds(r * group * chunks + c, group, stride=chunks), :]
            lhs[pl.ds(pl.multiple_of(r * group, group), group), c * LANES : (c + 1) * LANES] = piece.astype(jnp.bfloat16)
        return carry

    lax.fori_loop(0, rows // group, spread_lanes, 0)

    def project_up(k, carry):
        fetch(k).wait()
        both[k] = dot_t(gate_up[k], lhs[...])
        return carry

    lax.fori_loop(0, 2, project_up, 0)
    gate = both[0]
    hidden[...] = (gate / (1.0 + jnp.exp(-gate)) * both[1]).T.astype(jnp.bfloat16)
    step = wide // 4
    fetch_down.wait()

    def project_down(n, carry):
        part = down[:, pl.ds(pl.multiple_of(n * step, step), step)]
        made = jnp.dot(hidden[...], part, preferred_element_type=jnp.float32)
        for c in range(step // LANES):
            tiles[pl.ds(n * (step // LANES) + c, rows, stride=chunks), :] = made[:, c * LANES : (c + 1) * LANES]
        return carry

    lax.fori_loop(0, 4, project_down, 0)

    def settle(turn, carry):
        for out, target, target_step, source, source_step, size in moves:
            place = pl.multiple_of((source + turn * source_step) * chunks, chunks)
            piece = tiles[pl.ds(place, size * chunks), :].reshape(size, chunks, LANES)
            outs[out][pl.ds(target + turn * target_step, size)] = piece.astype(jnp.bfloat16)
        return carry

    lax.fori_loop(0, turns, settle, 0)


def run_experts(ins, w_gate_up, w_down, turns, moves, sizes):
    chunks = ins[0].shape[1]
    rows, wide, units = sum(b.shape[0] for b in ins), chunks * LANES, w_down.shape[1]
    return pl.pallas_call(
        functools.partial(experts_kernel, len(ins), turns, moves),
        in_specs=[whole(VMEM)] * len(ins) + [whole(pltpu.HBM)] * 2,
        out_specs=[whole(VMEM)] * len(sizes),
        out_shape=[jax.ShapeDtypeStruct((n, chunks, LANES), jnp.bfloat16) for n in sizes],
        scratch_shapes=[
            VMEM((rows, wide), jnp.bfloat16),
            VMEM((rows * chunks, LANES), jnp.float32),
            VMEM((2, units, rows), jnp.float32),
            VMEM((rows, units), jnp.bfloat16),
            VMEM(w_gate_up.shape[1:], jnp.bfloat16),
            VMEM(w_down.shape[1:], jnp.bfloat16),
            pltpu.SemaphoreType.DMA((3,)),
        ],
        compiler_params=pltpu.CompilerParams(vmem_limit_bytes=52 << 20),
        cost_estimate=pl.CostEstimate(
            flops=6 * rows * wide * units, bytes_accessed=6 * units * wide, transcendentals=rows * units
        ),
    )(*ins, w_gate_up, w_down)


def back_kernel(index, gates, *refs):
    boxes, (kept, out, tiles, box) = refs[:-4], refs[-4:]
    rows, chunks, _ = kept.shape
    start = 0
    for part in boxes:
        box[start : start + part.shape[0]] = part[...]
        start += part.shape[0]

    def token(t, carry):
        value = kept[t].astype(jnp.float32)
        for k in range(2):
            value = value + gates[2 * t + k] * box[index[2 * t + k]].astype(jnp.float32)
        tiles[pl.ds(pl.multiple_of(t * chunks, chunks), chunks), :] = value
        return carry

    lax.fori_loop(0, rows, token, 0, unroll=4)
    for c in range(chunks):
        out[:, c * LANES : (c + 1) * LANES] = tiles[pl.ds(c, rows, stride=chunks), :].astype(jnp.bfloat16)


def back(index, gates, boxes, kept):
    rows, chunks, _ = kept.shape
    total = sum(b.shape[0] for b in boxes)
    return pl.pallas_call(
        back_kernel,
        in_specs=[whole(SMEM)] * 2 + [whole(VMEM)] * (len(boxes) + 1),
        out_specs=whole(VMEM),
        out_shape=jax.ShapeDtypeStruct((rows, chunks * LANES), jnp.bfloat16),
        scratch_shapes=[VMEM((rows * chunks, LANES), jnp.float32), VMEM((total, chunks, LANES), jnp.bfloat16)],
        compiler_params=pltpu.CompilerParams(vmem_limit_bytes=LIMIT),
        cost_estimate=pl.CostEstimate(flops=1 << 20, bytes_accessed=1 << 22, transcendentals=0),
    )(index, gates, *boxes, kept)


def on_device(tokens, context, out_proj, norm_gain, router, expert_ids, w_gate_up, w_down):
    rows_here, width = tokens.shape
    columns = lax.axis_size("expert")
    members = lax.axis_size("fsdp")
    experts = columns * members // 2
    group = members // 2
    slot_cap = 5 * rows_here // (2 * experts)
    chunks = width // LANES
    assert group == 4

    def shift(even, odd):
        return [(i, (i + (odd if i % 2 else even)) % members) for i in range(members)]

    out_hops = (shift(-1, 1), shift(2, -2), shift(-3, 3))
    back_hops = tuple([(b, a) for a, b in hop] for hop in out_hops)
    swap = [(i, i ^ 1) for i in range(members)]

    def swapped(value):
        return lax.ppermute(value, "fsdp", swap)

    def spread(blocks, hops):
        return [blocks[0]] + [lax.ppermute(b, "fsdp", hop) for b, hop in zip(blocks[1:], hops)]

    def across(box):
        boxes = box.reshape(columns, -1, chunks, LANES)
        return lax.all_to_all(boxes, "expert", split_axis=0, concat_axis=0, tiled=True).reshape(box.shape)

    def split(box):
        parts = box.reshape(columns, group, -1, chunks, LANES)
        return [parts[:, m].reshape(-1, chunks, LANES) for m in range(group)]

    def join(blocks):
        parts = [b.reshape(columns, 1, -1, chunks, LANES) for b in blocks]
        return jnp.concatenate(parts, axis=1).reshape(-1, chunks, LANES)

    def add_halves(own, other):
        return (own.astype(jnp.float32) + other.astype(jnp.float32)).astype(jnp.bfloat16)

    here = lax.axis_index("fsdp")
    odd = here % 2
    depth = width // 2
    tokens_of = lambda h: lax.dynamic_slice_in_dim(tokens, h * depth, depth, axis=1)
    their_context = swapped(context)
    their_tokens = swapped(tokens_of(1 - odd))
    pieces = jnp.stack([out_proj[:, :depth], out_proj[:, depth:]])
    pieces = jnp.broadcast_to(pieces[None], (group,) + pieces.shape).reshape(members, -1, depth)
    pieces = lax.all_to_all(pieces, "fsdp", split_axis=0, concat_axis=0, tiled=True)
    block = pieces.reshape(-1, depth)
    hop = lambda value, by: lax.ppermute(value, "expert", [(i, (i + by) % columns) for i in range(columns)])
    twin = lambda value: lax.ppermute(value, "expert", [(i, i ^ 1) for i in range(columns)])
    upward, downward, held, offsets = [block], [block], [block], [(0, 0)]
    reach = columns // 4
    for k in range(1, reach):
        upward.append(hop(upward[-1], 2))
        downward.append(hop(downward[-1], -2))
        held.append(jnp.concatenate([upward[k], downward[k]], axis=0))
        offsets += [(-k, 0), (k, 0)]
    cut = block.shape[0] // 2
    ends = [hop(upward[-1][:cut], 2), hop(downward[-1][cut:], -2)]
    held.append(jnp.concatenate(ends, axis=0))
    offsets.append((reach, 0))
    held += [twin(v) for v in held]
    offsets = tuple(offsets + [(away, 1) for away, _ in offsets])
    position = lax.axis_index("expert").astype(jnp.int32).reshape(1)

    flat_ids, places = slot_places(expert_ids, experts)
    away = (flat_ids % group - here // 2) % group
    message = jnp.where(away == 0, 0, jnp.where(away == 2, 3, jnp.where((away == 1) == (odd == 0), 2, 1)))
    column = flat_ids // group
    cap_b = slot_cap // 2
    cap_a = slot_cap - cap_b
    lines = columns * group
    by_column = column * group + message
    by_message = message * columns + column
    early = places < cap_a
    first = lines * cap_a
    index_out = jnp.where(early, by_column * cap_a + places, first + by_message * cap_b + places - cap_a)
    index_in = jnp.where(early, by_message * cap_a + places, first + by_column * cap_b + places - cap_a)
    index_out, index_in = index_out.astype(jnp.int32), index_in.astype(jnp.int32)
    moves_a = tuple((0, m * cap_a, group * cap_a, m * columns * cap_a, cap_a, cap_a) for m in range(group))
    moves_b = tuple(
        (2 * d + (m > 0), max(m - 1, 0) * columns * cap_b, cap_b, (d * lines + m) * cap_b, group * cap_b, cap_b)
        for d in range(2)
        for m in range(group)
    )

    other = swapped(project(offsets, position, their_context, their_tokens, held))
    mine = project(offsets, position, context, tokens_of(odd), held)
    sizes = [lines * cap_a] + [columns * cap_b] * group
    box_a, boxes_b, kept, gates = front(
        index_out,
        odd.astype(jnp.int32).reshape(1),
        mine,
        other,
        norm_gain.reshape(1, width),
        router,
        expert_ids,
        sizes,
    )

    over_a = across(box_a)
    near_b = spread(boxes_b, out_hops)
    near_b = across(join(near_b))
    near_a = spread(split(over_a), out_hops)
    far_a = [swapped(near_a[0])]
    far_a += [swapped(b) for b in near_a[1:]]
    far_b = swapped(near_b)

    (own_a,) = run_experts(near_a, w_gate_up, w_down, columns, moves_a, [lines * cap_a])
    (other_a,) = run_experts(far_a, w_gate_up, w_down, columns, moves_a, [lines * cap_a])
    sum_a = add_halves(own_a, swapped(other_a))
    few = columns * cap_b
    made_b = run_experts([near_b, far_b], w_gate_up, w_down, columns, moves_b, [few, (group - 1) * few] * 2)
    going = add_halves(made_b[1], swapped(made_b[3]))
    staying = add_halves(made_b[0], swapped(made_b[2]))
    sum_b = [staying] + [going[m * few : (m + 1) * few] for m in range(group - 1)]
    sum_a = across(sum_a)
    sum_b = join(spread(sum_b, back_hops))
    done_b = across(sum_b)
    done_a = spread(split(sum_a), back_hops)
    return back(index_in, gates.reshape(-1), done_a + [done_b], kept)


def solution(mesh):
    rows = P(("sweep", "expert", "fsdp"), None)
    return jax.shard_map(
        on_device,
        mesh=mesh,
        in_specs=(
            rows,
            rows,
            rows,
            P("sweep"),
            P("sweep", None),
            rows,
            P(("sweep", "expert", "fsdp"), None, None, None),
            P(("sweep", "expert", "fsdp"), None, None),
        ),
        out_specs=rows,
        check_vma=False,
    )
```
